32 devices in a mesh: row: 8 (over z, x), col: 4 (over y, core).
Axes of the slice: x: 2, y: 2, z: 4, core: 2. Of those that a mesh axis runs over, the one named last changes fastest.
Arguments:
- tokens: bfloat16 [512, 12288], P('col', 'row'), may hold values from -16 to 16
- norm_gain: float32 [12288], P('row'), may hold values from 0.25 to 1.75
- weight_in: bfloat16 [12288, 49152], P('row', 'col'), may hold values from -0.0546875 to 0.0546875
- weight_out: bfloat16 [49152, 12288], P('col', 'row'), may hold values from -0.02734375 to 0.02734375
Outputs:
- mixed: bfloat16 [512, 12288], P('col', 'row')
The draws below stay inside these ranges and needn't reach their ends.
All inputs are finite; a program needn't handle non-finite values.
Results may differ from the reference program's by a relative error of at most 0.0051.
Values may be sent and summed in bfloat16 or wider, within the bound.
A program may use at most 192 MiB of HBM per device.

```python
import math
import jax
import jax.numpy as jnp
from jax import lax

D = 12288
FF = 49152
TOKENS = 512


def draw_tokens(key, part):
    base_key = jax.random.fold_in(key, 17)
    noise_key, col_key, row_key = jax.random.split(base_key, 3)
    position = jnp.arange(D, dtype=jnp.float32) / D
    col_scale = jnp.exp(math.log(3.0) * position + jax.random.uniform(col_key, (D,), jnp.float32, 0.0, math.log(3.0))) / 3.0
    row_scale = jnp.exp(jax.random.uniform(row_key, (TOKENS, 1), jnp.float32, math.log(0.1), 0.0))
    values = jax.random.normal(noise_key, (TOKENS, D), jnp.float32)
    return jnp.clip(values * row_scale * col_scale[None, :], -16.0, 16.0).astype(jnp.bfloat16)


def block_levels(rng, dims, pieces, smallest, largest):
    factor_of, own = 1.0, jax.random.fold_in(rng, 6)
    for dim, blocks in pieces:
        heights = jnp.exp(jax.random.uniform(jax.random.fold_in(own, dim), (blocks,), jnp.float32, smallest / len(pieces), largest / len(pieces)))
        factor_of = factor_of * jnp.repeat(heights, dims[dim] // blocks).reshape([-1 if axis == dim else 1 for axis in range(len(dims))])
    return factor_of


def centred(rng, dims, deviation, limit, cuts=(), held_as=jnp.bfloat16):
    factor_of = block_levels(rng, dims, cuts, -0.22, 0.18) if cuts else 1.0
    result = jax.random.normal(rng, dims, jnp.float32) * deviation * factor_of
    return jnp.minimum(jnp.maximum(result, -limit), limit).astype(held_as)


def setup_inputs(seed: int = 0) -> dict:
    key_of = jax.random.split(jax.random.key(seed), 5)
    tokens = draw_tokens(jax.random.fold_in(key_of[4], 71), 0)
    norm_gain = jnp.clip(1.0 + 0.15 * jax.random.normal(key_of[1], (D,), jnp.float32), 0.25, 1.75)
    weight_in = centred(key_of[2], (D, FF), D ** -0.5, 0.0546875, ((0, 8), (1, 4)))
    weight_out = centred(key_of[3], (FF, D), FF ** -0.5, 0.02734375, ((0, 4), (1, 8)))
    return {"tokens": tokens, "norm_gain": norm_gain, "weight_in": weight_in, "weight_out": weight_out}


epsilon = 1e-05

def reference(tokens, norm_gain, weight_in, weight_out):
    wide_input = tokens.astype(jnp.float32)
    scaled = (wide_input * norm_gain.astype(jnp.float32)[None, :]).astype(jnp.bfloat16)
    squares = lax.optimization_barrier(jnp.sum(wide_input * wide_input, axis=1))
    inverse = lax.rsqrt(squares / D + epsilon)
    hidden = jnp.dot(scaled, weight_in, preferred_element_type=jnp.float32) * inverse[:, None]
    active = jax.nn.gelu(hidden, approximate=True).astype(jnp.bfloat16)
    branch = jnp.dot(active, weight_out, preferred_element_type=jnp.float32)
    return (wide_input + branch).astype(jnp.bfloat16)
```

```python
import jax
import jax.numpy as jnp
from jax import lax
from jax.sharding import PartitionSpec as P

epsilon = 1e-05


def make(mesh):
    rows = mesh.shape["row"]

    def per_device(tokens, norm_gain, weight_in, weight_out):
        width = weight_in.shape[0] * rows
        gathered = lax.all_gather(tokens, "col", axis=0, tiled=True)
        wide_input = gathered.astype(jnp.float32)
        scaled = (wide_input * norm_gain[None, :]).astype(jnp.bfloat16)
        squares = jnp.sum(wide_input * wide_input, axis=1)
        square_sum = squares
        for shift in range(1, rows):
            square_sum = square_sum + lax.ppermute(
                squares, "row", [(i, (i + shift) % rows) for i in range(rows)]
            )
        own = squares.shape[0] // rows
        square_sum = lax.dynamic_slice_in_dim(
            square_sum, lax.axis_index("row") * own, own
        )
        partial_value = jnp.dot(
            scaled, weight_in, preferred_element_type=jnp.float32
        ).astype(jnp.bfloat16)
        hidden_sum = lax.psum_scatter(
            partial_value, "row", scatter_dimension=0, tiled=True
        ).astype(jnp.float32)
        inverse = lax.rsqrt(square_sum / width + epsilon)
        hidden = hidden_sum * inverse[:, None]
        active = jax.nn.gelu(hidden, approximate=True).astype(jnp.bfloat16)
        branch = jnp.dot(
            lax.all_gather(active, "row", axis=0, tiled=True),
            weight_out,
            preferred_element_type=jnp.float32,
        ).astype(jnp.bfloat16)
        output_rows = lax.psum_scatter(
            branch, "col", scatter_dimension=0, tiled=True
        ).astype(jnp.float32)
        return (tokens.astype(jnp.float32) + output_rows).astype(jnp.bfloat16)

    return per_device


def solution(mesh):
    in_specs = (P("col", "row"), P("row"), P("row", "col"), P("col", "row"))
    out_specs = P("col", "row")
    return jax.shard_map(
        make(mesh), mesh=mesh, in_specs=in_specs, out_specs=out_specs, check_vma=False
    )
```
